32 devices in a mesh: grp: 8 (over z, x), sub: 4 (over y, core).
Axes of the slice: x: 2, y: 2, z: 4, core: 2. Of those that a mesh axis runs over, the one named last changes fastest.
Arguments:
- gate_source: bfloat16 [32, 2048, 768], P('grp', 'sub'), may hold values from -0.125 to 0.125
- up_source: bfloat16 [32, 2048, 768], P('grp', 'sub'), may hold values from -0.125 to 0.125
- down_source: bfloat16 [32, 2048, 768], P('grp', 'sub'), may hold values from -0.21875 to 0.21875
- source_order: int32 [32], replicated, may hold values from 0 to 31, each once
- target_order: int32 [32], replicated, may hold values from 0 to 31, each once
Outputs:
- packed: bfloat16 [3, 8, 4, 8, 96, 2048], P(None, 'grp', 'sub')
- scales: float32 [3, 8, 4, 16, 768], P(None, 'grp', 'sub')
The draws below stay inside these ranges and needn't reach their ends.
Inputs may be any that keep to these rules, and one draw needn't show every extreme that they name: `source_order`: each expert number appears once. `target_order`: each expert number appears once.
All inputs are finite; a program needn't handle non-finite values. Where the reference program divides by a largest or mean magnitude, that divisor is 1e-20 or more.
Results may differ from the reference program's by a relative error of at most 0.001.
Values may be sent and summed in bfloat16 or wider, within the bound.
No kernel may reach another device: no remote copies, remote signals or barrier semaphores. Data moves between devices by JAX's collectives and lax.ppermute only.
A program may use at most 192 MiB of HBM per device.

```python
import jax
import jax.numpy as jnp
from jax import lax

D = 2048
FF = 768
BLOCK = 128
E = 32
EPT = 8
FFT = 96
N_GRP = 8
N_SUB = 4


def levels(rng, shape, shards, smallest, largest):
    def one(position, blocks):
        steps = jax.random.uniform(jax.random.fold_in(jax.random.fold_in(rng, 6), position), (blocks,), jnp.float32, smallest / len(shards), largest / len(shards))
        return jnp.repeat(jnp.exp(steps), shape[position] // blocks).reshape((-1,) + (1,) * (len(shape) - position - 1))

    level = one(*shards[0])
    for cut in shards[1:]:
        level = level * one(*cut)
    return level


def bell_draw(own_key, shape, spread, most, cuts=(), kind=jnp.bfloat16):
    entries = spread * jax.random.normal(own_key, shape, jnp.float32)
    if cuts:
        entries = entries * levels(own_key, shape, cuts, -0.22, 0.18)
    return jnp.clip(entries, -most, most).astype(kind)


def setup_inputs(seed: int = 0) -> dict:
    splits = jax.random.split(jax.random.key(seed), 6)
    return {
        "gate_source": bell_draw(splits[0], (E, D, FF), D ** -0.5, 0.125, ((0, 8), (1, 4))),
        "up_source": bell_draw(splits[1], (E, D, FF), D ** -0.5, 0.125, ((0, 8), (1, 4))),
        "down_source": bell_draw(splits[2], (E, D, FF), FF ** -0.5, 0.21875, ((0, 8), (1, 4))),
        "source_order": jax.random.permutation(splits[3], E).astype(jnp.int32),
        "target_order": jax.random.permutation(splits[4], E).astype(jnp.int32),
    }


EPS = 1e-6


def pack_layout(quantized):
    values = quantized.reshape(N_GRP // 2, EPT, D, 2, N_SUB, FFT)
    values = values.transpose(0, 3, 4, 1, 5, 2)
    return values.reshape(N_GRP, N_SUB, EPT, FFT, D)


def scale_layout(block_scale):
    values = block_scale.reshape(N_GRP // 2, EPT, D // BLOCK, 2, N_SUB, FFT)
    values = values.transpose(0, 3, 4, 2, 1, 5)
    return values.reshape(N_GRP, N_SUB, D // BLOCK, EPT * FFT)


def convert(weights, picked):
    def convert_one(target):
        matrix = weights[picked[target]].astype(jnp.float32).reshape(D // BLOCK, BLOCK, FF)
        block_scale = jnp.max(jnp.abs(matrix), axis=1) + EPS
        quantized = (matrix / block_scale[:, None, :]).astype(jnp.bfloat16).reshape(D, FF)
        return quantized, block_scale

    quantized, block_scale = lax.map(convert_one, jnp.arange(E, dtype=jnp.int32))
    return pack_layout(quantized), scale_layout(block_scale)


def reference(gate_source, up_source, down_source, source_order, target_order):
    matches = (source_order[None, :] == target_order[:, None]).astype(jnp.int32)
    picked = jnp.sum(matches * jnp.arange(E, dtype=jnp.int32)[None, :], axis=1).astype(jnp.int32)
    gate_q, gate_s = convert(gate_source, picked)
    up_q, up_s = convert(up_source, picked)
    down_q, down_s = convert(down_source, picked)
    return jnp.stack([gate_q, up_q, down_q]), jnp.stack([gate_s, up_s, down_s])
```

```python
import functools

import jax
import jax.numpy as jnp
from jax import lax
from jax.experimental import pallas as pl
from jax.experimental.pallas import tpu as pltpu
from jax.sharding import Mesh, PartitionSpec as P

BLOCK = 128
EPS = 1e-06
STATIC_ROUNDS = 6


def plan_kernel(source_order, target_order, send, place, own, rounds, where_is, code, queue, size, line,
                *, targets, per_group, limit):
    experts = targets * per_group

    def note(j, c):
        where_is[target_order[j]] = j
        own[j // per_group, j % per_group] = 0
        return c

    lax.fori_loop(0, experts, note, 0)

    def look(p, c):
        j = where_is[source_order[p]]
        code[p] = j
        t = p // per_group
        stays = (j // per_group) == t

        @pl.when(stays)
        def _():
            own[t, j % per_group] = p % per_group

        return c

    lax.fori_loop(0, experts, look, 0)
    rounds[0] = 0
    for d in range(2):

        def order(t, c, d=d):
            size[t] = 0
            line[t] = -1

            def reach(e, c2):
                dest = (targets - 1 - e) if d == 0 else e

                @pl.when((dest > t) if d == 0 else (dest < t))
                def _():
                    def pick(i, c3):
                        p = t * per_group + i

                        @pl.when(code[p] // per_group == dest)
                        def _():
                            queue[t * per_group + size[t]] = p
                            size[t] = size[t] + 1

                        return c3

                    lax.fori_loop(0, per_group, pick, 0)

                return c2

            lax.fori_loop(0, targets, reach, 0)
            where_is[t] = 0
            return c

        lax.fori_loop(0, targets, order, 0)

        def step(r, c, d=d):
            def at(e, c2):
                t = (targets - 1 - e) if d == 0 else e
                held = line[t]
                dest = jnp.where(held >= 0, code[jnp.maximum(held, 0)] // per_group, t)
                passes = (dest != t) & (held >= 0)
                front = where_is[t]
                fresh = jnp.logical_not(passes) & (front < size[t])
                slot = queue[jnp.minimum(t * per_group + front, experts - 1)]
                where_is[t] = front + jnp.where(fresh, 1, 0)
                sent = jnp.where(passes, held, jnp.where(fresh, slot, -1))
                send[d * targets + t, r] = jnp.where(fresh, slot - t * per_group, jnp.where(passes, -1, 0))
                nxt = t + 1 if d == 0 else t - 1

                @pl.when((nxt < targets) & (nxt >= 0))
                def _():
                    line[nxt] = sent
                    j = code[jnp.maximum(sent, 0)]
                    mine = (sent >= 0) & (j // per_group == nxt)
                    place[d * targets + nxt, r] = jnp.where(mine, j % per_group, per_group)

                    @pl.when(sent >= 0)
                    def _():
                        rounds[0] = jnp.maximum(rounds[0], r + 1)

                return c2

            lax.fori_loop(0, targets, at, 0)
            first = 0 if d == 0 else targets - 1
            place[d * targets + first, r] = per_group
            line[first] = -1
            return c

        lax.fori_loop(0, limit, step, 0)


def make_plan(source_order, target_order, targets, per_group):
    experts = targets * per_group
    limit = experts // 2 + targets + STATIC_ROUNDS
    smem = pl.BlockSpec(memory_space=pltpu.SMEM)
    return pl.pallas_call(
        functools.partial(plan_kernel, targets=targets, per_group=per_group, limit=limit),
        out_shape=(
            jax.ShapeDtypeStruct((2 * targets, limit), jnp.int32),
            jax.ShapeDtypeStruct((2 * targets, limit), jnp.int32),
            jax.ShapeDtypeStruct((targets, per_group), jnp.int32),
            jax.ShapeDtypeStruct((1,), jnp.int32),
        ),
        in_specs=[smem, smem],
        out_specs=(smem, smem, smem, smem),
        scratch_shapes=[
            pltpu.SMEM((experts,), jnp.int32),
            pltpu.SMEM((experts,), jnp.int32),
            pltpu.SMEM((experts,), jnp.int32),
            pltpu.SMEM((targets,), jnp.int32),
            pltpu.SMEM((targets,), jnp.int32),
        ],
        cost_estimate=pl.CostEstimate(flops=1000, bytes_accessed=20_000_000, transcendentals=0),
        name="plan",
    )(source_order, target_order)


def turn(weights, splits):
    slots, rows, hidden = weights.shape
    columns = hidden // splits

    def kernel(x, out):
        out[...] = x[0].T.reshape(splits, 1, columns, rows)

    return pl.pallas_call(
        kernel,
        grid=(slots,),
        in_specs=[pl.BlockSpec((1, rows, hidden), lambda i: (i, 0, 0))],
        out_specs=pl.BlockSpec((splits, 1, columns, rows), lambda i: (0, i, 0, 0)),
        out_shape=jax.ShapeDtypeStruct((splits, slots, columns, rows), weights.dtype),
        cost_estimate=pl.CostEstimate(flops=0, bytes_accessed=4 * weights.size, transcendentals=0),
        name="turn",
    )(weights)


def keep(held, own):
    halves, shards, slots, columns, rows = held.shape
    per_group = halves * slots

    def kernel(index, x, out):
        out[...] = x[0, :, 0][None]

    return pl.pallas_call(
        kernel,
        grid_spec=pltpu.PrefetchScalarGridSpec(
            num_scalar_prefetch=1,
            grid=(per_group,),
            in_specs=[pl.BlockSpec((1, shards, 1, columns, rows), lambda k, index: (index[k] // slots, 0, index[k] % slots, 0, 0))],
            out_specs=pl.BlockSpec((1, shards, columns, rows), lambda k, index: (k, 0, 0, 0)),
        ),
        out_shape=jax.ShapeDtypeStruct((per_group + 1, shards, columns, rows), held.dtype),
        cost_estimate=pl.CostEstimate(flops=0, bytes_accessed=4 * held.size, transcendentals=0),
        name="keep",
    )(own, held)


def scale_all(staged, per_group):
    matrices = len(staged)
    _, shards, columns, rows = staged[0].shape
    blocks = rows // BLOCK

    def kernel(*refs):
        ins, out, scales = refs[:matrices], refs[matrices], refs[matrices + 1]
        for m in range(matrices):
            tops = []
            for s in range(shards):
                for b in range(blocks):
                    v = ins[m][0, s, :, b * BLOCK:(b + 1) * BLOCK].astype(jnp.float32)
                    top = jnp.max(jnp.abs(v), axis=1, keepdims=True) + EPS
                    n = s * blocks + b
                    out[m, 0, :, n * BLOCK:(n + 1) * BLOCK] = (v * (1.0 / top)).astype(out.dtype)
                    tops.append(top)
            scales[m, 0] = jnp.concatenate(tops, axis=1).T

    return pl.pallas_call(
        kernel,
        grid=(per_group,),
        in_specs=[pl.BlockSpec((1, shards, columns, rows), lambda k: (k, 0, 0, 0))] * matrices,
        out_specs=(
            pl.BlockSpec((matrices, 1, columns, shards * rows), lambda k: (0, k, 0, 0)),
            pl.BlockSpec((matrices, 1, shards * blocks, columns), lambda k: (0, k, 0, 0)),
        ),
        out_shape=(
            jax.ShapeDtypeStruct((matrices, per_group, columns, shards * rows), jnp.bfloat16),
            jax.ShapeDtypeStruct((matrices, per_group, shards * blocks, columns), jnp.float32),
        ),
        name="scale",
    )(*staged)


def per_device(gate_source, up_source, down_source, source_order, target_order):
    targets = lax.axis_size("t")
    halves = lax.axis_size("h")
    shards = lax.axis_size("sub")
    splits = halves * shards
    slots, rows, hidden = gate_source.shape
    per_group = halves * slots
    columns = hidden // splits
    me = lax.axis_index("t")
    send, place, own, rounds = make_plan(source_order, target_order, targets, per_group)
    send = send.reshape(2, targets, -1)[:, me]
    place = place.reshape(2, targets, -1)[:, me]
    own = own[me]
    ways = ([(i, i + 1) for i in range(targets - 1)], [(i + 1, i) for i in range(targets - 1)])

    held, staged = [], []
    for weights in (gate_source, up_source, down_source):
        pieces = turn(weights, splits)
        got = lax.all_to_all(pieces, ("h", "sub"), split_axis=0, concat_axis=0, tiled=True)
        got = got.reshape(halves, shards, slots, columns, rows)
        held.append(got)
        staged.append(keep(got, own))

    def one_round(r, whole, stage, last):
        new = []
        for d in range(2):
            index = send[d, r]
            at = jnp.maximum(index, 0)
            fresh = lax.dynamic_slice(
                whole, (at // slots, 0, at % slots, 0, 0), (1, shards, 1, columns, rows)
            ).reshape(shards, columns, rows)
            if last is not None:
                fresh = jnp.where(index < 0, last[d], fresh)
            new.append(lax.ppermute(fresh, "t", ways[d]))
        for d in range(2):
            stage = lax.dynamic_update_slice(stage, new[d][None], (place[d, r], 0, 0, 0))
        return stage, tuple(new)

    matrices = len(held)
    last = [None] * matrices
    for m in range(matrices):
        for r in range(STATIC_ROUNDS):
            staged[m], last[m] = one_round(r, held[m], staged[m], last[m])

    def more(carry):
        return carry[0] < rounds[0]

    def go(carry):
        r, stage, prior = carry
        out = [one_round(r, held[m], stage[m], prior[m]) for m in range(matrices)]
        return r + 1, tuple(o[0] for o in out), tuple(o[1] for o in out)

    _, staged, _ = lax.while_loop(more, go, (jnp.int32(STATIC_ROUNDS), tuple(staged), tuple(last)))
    packed, scales = scale_all(list(staged), per_group)
    packed = packed.reshape(matrices, 1, 1, per_group, columns, shards * rows)
    scales = scales.transpose(0, 2, 1, 3).reshape(matrices, 1, 1, -1, per_group * columns)
    return packed, scales


def solution(mesh):
    groups, shards = mesh.devices.shape
    fine = Mesh(mesh.devices.reshape(groups // 2, 2, shards), ("t", "h", "sub"))
    spec = P(("t", "h"), "sub", None)
    return jax.shard_map(
        per_device,
        mesh=fine,
        in_specs=(spec, spec, spec, P(), P()),
        out_specs=(P(None, ("t", "h"), "sub", None, None, None), P(None, ("t", "h"), "sub", None, None)),
        check_vma=False,
    )
```

```python
import functools

import jax
import jax.numpy as jnp
from jax import lax
from jax.experimental import pallas as pl
from jax.experimental.pallas import tpu as pltpu
from jax.sharding import Mesh, PartitionSpec as P


BLOCK = 128
EPS = 1e-06
STATIC_ROUNDS = 8


def plan_kernel(source_order, target_order, me, half, slot, passed, place, own, rounds, where_is, code, queue, size, line,
                *, targets, per_group, slots, limit):
    experts = targets * per_group

    def note(j, c):
        where_is[target_order[j]] = j
        return c

    lax.fori_loop(0, experts, note, 0)
    for k in range(per_group):
        own[0, k] = 0
        own[1, k] = 0

    def look(p, c):
        j = where_is[source_order[p]]
        code[p] = j
        t = p // per_group

        @pl.when((j // per_group == t) & (t == me[0]))
        def _():
            own[0, j % per_group] = (p % per_group) // slots
            own[1, j % per_group] = p % slots

        return c

    lax.fori_loop(0, experts, look, 0)
    rounds[0] = 0
    for d in range(2):

        def order(t, c, d=d):
            size[t] = 0
            line[t] = -1

            def reach(e, c2):
                dest = (targets - 1 - e) if d == 0 else e

                @pl.when((dest > t) if d == 0 else (dest < t))
                def _():
                    def pick(i, c3):
                        p = t * per_group + i

                        @pl.when(code[p] // per_group == dest)
                        def _():
                            queue[t * per_group + size[t]] = p
                            size[t] = size[t] + 1

                        return c3

                    lax.fori_loop(0, per_group, pick, 0)

                return c2

            lax.fori_loop(0, targets, reach, 0)
            where_is[t] = 0
            return c

        lax.fori_loop(0, targets, order, 0)

        def step(r, c, d=d):
            def at(e, c2):
                t = (targets - 1 - e) if d == 0 else e
                held = line[t]
                dest = jnp.where(held >= 0, code[jnp.maximum(held, 0)] // per_group, t)
                passes = (dest != t) & (held >= 0)
                front = where_is[t]
                fresh = jnp.logical_not(passes) & (front < size[t])
                chosen = queue[jnp.minimum(t * per_group + front, experts - 1)]
                where_is[t] = front + jnp.where(fresh, 1, 0)
                sent = jnp.where(passes, held, jnp.where(fresh, chosen, -1))

                @pl.when(t == me[0])
                def _():
                    i = jnp.where(fresh, chosen - t * per_group, 0)
                    half[d, r] = i // slots
                    slot[d, r] = i % slots
                    passed[d, r] = jnp.where(passes, 1, 0)

                nxt = t + 1 if d == 0 else t - 1

                @pl.when((nxt < targets) & (nxt >= 0))
                def _():
                    line[nxt] = sent
                    j = code[jnp.maximum(sent, 0)]
                    mine = (sent >= 0) & (j // per_group == nxt)

                    @pl.when(nxt == me[0])
                    def _():
                        place[d, r] = jnp.where(mine, j % per_group, per_group)

                    @pl.when(sent >= 0)
                    def _():
                        rounds[0] = jnp.maximum(rounds[0], r + 1)

                return c2

            lax.fori_loop(0, targets, at, 0)
            first = 0 if d == 0 else targets - 1

            @pl.when(first == me[0])
            def _():
                place[d, r] = per_group

            line[first] = -1
            return c

        lax.fori_loop(0, limit, step, 0)


def make_plan(source_order, target_order, me, targets, per_group, slots):
    experts = targets * per_group
    limit = experts // 2 + targets + STATIC_ROUNDS
    smem = pl.BlockSpec(memory_space=pltpu.SMEM)
    row = jax.ShapeDtypeStruct((2, limit), jnp.int32)
    return pl.pallas_call(
        functools.partial(plan_kernel, targets=targets, per_group=per_group, slots=slots, limit=limit),
        out_shape=(
            row, row, row, row,
            jax.ShapeDtypeStruct((2, per_group), jnp.int32),
            jax.ShapeDtypeStruct((1,), jnp.int32),
        ),
        in_specs=[smem] * 3,
        out_specs=(smem,) * 6,
        scratch_shapes=[
            pltpu.SMEM((experts,), jnp.int32),
            pltpu.SMEM((experts,), jnp.int32),
            pltpu.SMEM((experts,), jnp.int32),
            pltpu.SMEM((targets,), jnp.int32),
            pltpu.SMEM((targets,), jnp.int32),
        ],
        cost_estimate=pl.CostEstimate(flops=1000, bytes_accessed=20_000_000, transcendentals=0),
        name="plan",
    )(source_order, target_order, me.reshape(1))


def turn(weights, splits):
    slots, rows, hidden = weights.shape
    columns = hidden // splits

    def kernel(x, out):
        out[...] = x[0].T.reshape(splits, 1, columns, rows)

    return pl.pallas_call(
        kernel,
        grid=(slots,),
        in_specs=[pl.BlockSpec((1, rows, hidden), lambda i: (i, 0, 0))],
        out_specs=pl.BlockSpec((splits, 1, columns, rows), lambda i: (0, i, 0, 0)),
        out_shape=jax.ShapeDtypeStruct((splits, slots, columns, rows), weights.dtype),
        cost_estimate=pl.CostEstimate(flops=0, bytes_accessed=4 * weights.size, transcendentals=0),
        name="turn",
    )(weights)


def keep(held, own):
    halves, shards, slots, columns, rows = held.shape
    per_group = halves * slots

    def kernel(index, x, out):
        out[...] = x[0, :, 0][None]

    return pl.pallas_call(
        kernel,
        grid_spec=pltpu.PrefetchScalarGridSpec(
            num_scalar_prefetch=1,
            grid=(per_group,),
            in_specs=[pl.BlockSpec((1, shards, 1, columns, rows), lambda k, index: (index[0, k], 0, index[1, k], 0, 0))],
            out_specs=pl.BlockSpec((1, shards, columns, rows), lambda k, index: (k, 0, 0, 0)),
        ),
        out_shape=jax.ShapeDtypeStruct((per_group + 1, shards, columns, rows), held.dtype),
        cost_estimate=pl.CostEstimate(flops=0, bytes_accessed=4 * held.size, transcendentals=0),
        name="keep",
    )(own, held)


def scale_all(staged, per_group):
    matrices = len(staged)
    _, shards, columns, rows = staged[0].shape
    blocks = rows // BLOCK

    def kernel(*refs):
        ins, out, scales = refs[:matrices], refs[matrices], refs[matrices + 1]
        for m in range(matrices):
            tops = []
            for s in range(shards):
                for b in range(blocks):
                    v = ins[m][0, s, :, b * BLOCK:(b + 1) * BLOCK].astype(jnp.float32)
                    top = jnp.max(jnp.abs(v), axis=1, keepdims=True) + EPS
                    n = s * blocks + b
                    out[m, 0, :, n * BLOCK:(n + 1) * BLOCK] = (v * (1.0 / top)).astype(out.dtype)
                    tops.append(top)
            scales[m, 0] = jnp.concatenate(tops, axis=1).T

    return pl.pallas_call(
        kernel,
        grid=(per_group,),
        in_specs=[pl.BlockSpec((1, shards, columns, rows), lambda k: (k, 0, 0, 0))] * matrices,
        out_specs=(
            pl.BlockSpec((matrices, 1, columns, shards * rows), lambda k: (0, k, 0, 0)),
            pl.BlockSpec((matrices, 1, shards * blocks, columns), lambda k: (0, k, 0, 0)),
        ),
        out_shape=(
            jax.ShapeDtypeStruct((matrices, per_group, columns, shards * rows), jnp.bfloat16),
            jax.ShapeDtypeStruct((matrices, per_group, shards * blocks, columns), jnp.float32),
        ),
        name="scale",
    )(*staged)


def regroup(gate_source, up_source, down_source, source_order, target_order):
    targets = lax.axis_size("t")
    halves = lax.axis_size("h")
    shards = lax.axis_size("sub")
    splits = halves * shards
    slots, rows, hidden = gate_source.shape
    per_group = halves * slots
    columns = hidden // splits
    me = lax.axis_index("t")
    half, slot, passed, place, own, rounds = make_plan(
        source_order, target_order, me.astype(jnp.int32), targets, per_group, slots
    )
    ways = ([(i, i + 1) for i in range(targets - 1)], [(i + 1, i) for i in range(targets - 1)])

    held, staged = [], []
    for weights in (gate_source, up_source, down_source):
        if held:
            weights, half, slot, passed, place, own, rounds = lax.optimization_barrier(
                (weights, half, slot, passed, place, own, rounds)
            )
        pieces = turn(weights, splits)
        if held:
            pieces, held[-1] = lax.optimization_barrier((pieces, held[-1]))
        got = lax.all_to_all(pieces, ("h", "sub"), split_axis=0, concat_axis=0, tiled=True)
        got = got.reshape(halves, shards, slots, columns, rows)
        held.append(got)
        staged.append(keep(got, own))

    def at(table, d, r):
        if isinstance(r, int):
            return table[d, r]
        return lax.dynamic_index_in_dim(table[d], r, keepdims=False, allow_negative_indices=False)

    def one_round(r, whole, stage, last):
        new = []
        for d in range(2):
            fresh = lax.dynamic_slice(
                whole, (at(half, d, r), 0, at(slot, d, r), 0, 0), (1, shards, 1, columns, rows),
                allow_negative_indices=False,
            )
            if last is not None:
                fresh = jnp.where(at(passed, d, r) > 0, last[d], fresh)
            new.append(lax.ppermute(fresh, "t", ways[d]))
        for d in range(2):
            stage = lax.dynamic_update_slice(
                stage, new[d].reshape(1, shards, columns, rows), (at(place, d, r), 0, 0, 0),
                allow_negative_indices=False,
            )
        return stage, tuple(new)

    matrices = len(held)
    last = [None] * matrices
    for m in range(matrices):
        for r in range(STATIC_ROUNDS):
            staged[m], last[m] = one_round(r, held[m], staged[m], last[m])

    def more(carry):
        return carry[0] < rounds[0]

    def go(carry):
        r, stage, prior = carry
        out = [one_round(r, held[m], stage[m], prior[m]) for m in range(matrices)]
        return r + 1, tuple(o[0] for o in out), tuple(o[1] for o in out)

    _, staged, _ = lax.while_loop(more, go, (jnp.int32(STATIC_ROUNDS), tuple(staged), tuple(last)))
    packed, scales = scale_all(list(staged), per_group)
    packed = packed.reshape(matrices, 1, 1, per_group, columns, shards * rows)
    scales = scales.transpose(0, 2, 1, 3).reshape(matrices, 1, 1, -1, per_group * columns)
    return packed, scales


def solution(mesh):
    groups, shards = mesh.devices.shape
    fine = Mesh(mesh.devices.reshape(groups // 2, 2, shards), ("t", "h", "sub"))
    spec = P(("t", "h"), "sub", None)
    return jax.shard_map(
        regroup,
        mesh=fine,
        in_specs=(spec, spec, spec, P(), P()),
        out_specs=(P(None, ("t", "h"), "sub", None, None, None), P(None, ("t", "h"), "sub", None, None)),
        check_vma=False,
    )
```
